32 devices in a mesh: dp: 4 (over y, z), tp: 8 (over x, core).
Axes of the slice: x: 4, y: 2, z: 2, core: 2. Of those that a mesh axis runs over, the one named last changes fastest.
The devices are a block of a 4x4x8 slice.
Arguments:
- x_in: bfloat16 [2304, 4096], P(('dp', 'tp')), parts along dimension 0
- req_ids: int32 [2304], P('dp'), parts along dimension 0
- positions: int32 [2304], P('dp'), parts along dimension 0
- block_table: int32 [260, 64], P('dp'), parts along dimension 0
- ctx_len: int32 [260], P('dp'), parts along dimension 0
- k_pages: bfloat16 [4352, 16, 8, 128], P('dp', None, 'tp'), parts along dimension 0
- v_pages: bfloat16 [4352, 16, 8, 128], P('dp', None, 'tp'), parts along dimension 0
- w_q: bfloat16 [4096, 4096], P(None, 'tp')
- w_k: bfloat16 [4096, 1024], P(None, 'tp')
- w_v: bfloat16 [4096, 1024], P(None, 'tp')
- w_o: bfloat16 [4096, 4096], P('tp')
- w_gate: bfloat16 [4096, 14336], P(None, 'tp')
- w_up: bfloat16 [4096, 14336], P(None, 'tp')
- w_down: bfloat16 [14336, 4096], P('tp')
- g_attn: bfloat16 [4096], replicated
- g_mlp: bfloat16 [4096], replicated
Outputs:
- output 1: bfloat16 [2304, 4096], P(('dp', 'tp')), parts along dimension 0
- output 2: bfloat16 [4352, 16, 8, 128], P('dp', None, 'tp'), parts along dimension 0
- output 3: bfloat16 [4352, 16, 8, 128], P('dp', None, 'tp'), parts along dimension 0
There are 4 independent parts. The reference program is written for one: setup_inputs(seed, part) draws one part's arguments, and reference() takes and returns one part's arrays. A program takes and returns all parts, laid end to end along the dimension named above; an argument that names none is the same for every part.
All inputs are finite; a program needn't handle non-finite values.
Results may differ from the reference program's by a relative error of at most 0.017261.
Values are sent between devices in bfloat16 or wider.
A program may use at most 768 MiB of HBM per device.

```python
import jax
import jax.numpy as jnp
from jax import lax

D_MODEL = 4096
HEADS = 32
KV_HEADS = 8
HEAD = 128
FF = 14336
CHUNK = 512
DECODE = 64
PREFIX = 512
DEC_CTX = 256
PAGE = 16
QUERY_BLOCK = 128
DECODE_BLOCK = 8

EPS = 1e-5
THETA = 500000.0
K_SCALE = 2.5
V_SCALE = 1.5
TOKENS = CHUNK + DECODE
REQS = DECODE + 1
CHUNK_PAGES = (PREFIX + CHUNK) // PAGE
DEC_PAGES = DEC_CTX // PAGE
TABLE_WIDTH = max(CHUNK_PAGES, DEC_PAGES)
POOL = CHUNK_PAGES + DECODE * DEC_PAGES
GROUP_REP = HEADS // KV_HEADS


def draw_layout(layout_key):
    subkeys = jax.random.split(layout_key, 5)
    req_order = jax.random.permutation(subkeys[0], REQS).astype(jnp.int32)
    dec_len = jax.random.randint(subkeys[1], (DECODE,), DEC_CTX // 4, DEC_CTX + 1, dtype=jnp.int32)
    longest = jax.random.randint(subkeys[2], (), 0, DECODE, dtype=jnp.int32)
    dec_len = jnp.where(jnp.arange(DECODE) == longest, DEC_CTX, dec_len).astype(jnp.int32)
    slot_len = jnp.concatenate([jnp.full((1,), PREFIX + CHUNK, jnp.int32), dec_len])
    inverse = jnp.argsort(req_order)
    ctx_len = slot_len[inverse]
    req_ids = jnp.concatenate([jnp.full((CHUNK,), req_order[0], jnp.int32), req_order[1:]])
    positions = jnp.concatenate([PREFIX + jnp.arange(CHUNK, dtype=jnp.int32), dec_len - 1])
    page_order = jax.random.permutation(subkeys[3], POOL).astype(jnp.int32)
    slot_table = jax.random.randint(subkeys[4], (REQS, TABLE_WIDTH), 0, POOL, dtype=jnp.int32)
    slot_table = slot_table.at[0, :CHUNK_PAGES].set(page_order[:CHUNK_PAGES])
    slot_table = slot_table.at[1:, :DEC_PAGES].set(page_order[CHUNK_PAGES:].reshape(DECODE, DEC_PAGES))
    block_table = slot_table[inverse]
    return req_ids, positions, block_table, ctx_len


def draw_dense(weight_key, fan_in, fan_out, gain):
    return (gain * fan_in ** -0.5 * jax.random.normal(weight_key, (fan_in, fan_out), jnp.float32)).astype(jnp.bfloat16)


def setup_inputs(seed: int = 0, part: int = 0) -> dict:
    base_key = jax.random.key(seed)
    part_keys = jax.random.split(jax.random.fold_in(base_key, part), 4)
    weight_keys = jax.random.split(base_key, 9)
    req_ids, positions, block_table, ctx_len = draw_layout(part_keys[0])
    cache_shape = (POOL, PAGE, KV_HEADS, HEAD)
    return {
        'x_in': jax.random.normal(part_keys[1], (TOKENS, D_MODEL), jnp.float32).astype(jnp.bfloat16),
        'req_ids': req_ids,
        'positions': positions,
        'block_table': block_table,
        'ctx_len': ctx_len,
        'k_pages': (K_SCALE * jax.random.normal(part_keys[2], cache_shape, jnp.float32)).astype(jnp.bfloat16),
        'v_pages': (V_SCALE * jax.random.normal(part_keys[3], cache_shape, jnp.float32)).astype(jnp.bfloat16),
        'w_q': draw_dense(weight_keys[0], D_MODEL, HEADS * HEAD, 1.0),
        'w_k': draw_dense(weight_keys[1], D_MODEL, KV_HEADS * HEAD, K_SCALE),
        'w_v': draw_dense(weight_keys[2], D_MODEL, KV_HEADS * HEAD, V_SCALE),
        'w_o': draw_dense(weight_keys[3], HEADS * HEAD, D_MODEL, 1.0),
        'w_gate': draw_dense(weight_keys[4], D_MODEL, FF, 1.0),
        'w_up': draw_dense(weight_keys[5], D_MODEL, FF, 1.0),
        'w_down': draw_dense(weight_keys[6], FF, D_MODEL, 1.0),
        'g_attn': jax.random.uniform(weight_keys[7], (D_MODEL,), jnp.float32, 0.5, 1.5).astype(jnp.bfloat16),
        'g_mlp': jax.random.uniform(weight_keys[8], (D_MODEL,), jnp.float32, 0.5, 1.5).astype(jnp.bfloat16),
    }


def rms_norm(rows, gain):
    rows32 = rows.astype(jnp.float32)
    inv_rms = lax.rsqrt(jnp.mean(rows32 * rows32, axis=-1, keepdims=True) + EPS)
    return (rows32 * inv_rms * gain.astype(jnp.float32)).astype(jnp.bfloat16)


def rotary(vals, positions):
    half_dim = vals.shape[-1] // 2
    inv_freq = THETA ** (-jnp.arange(half_dim, dtype=jnp.float32) * 2.0 / vals.shape[-1])
    angles = positions.astype(jnp.float32)[:, None] * inv_freq[None, :]
    cosine = jnp.cos(angles)[:, None, :]
    sine_val = jnp.sin(angles)[:, None, :]
    vals32 = vals.astype(jnp.float32)
    first_half = vals32[..., :half_dim]
    second_half = vals32[..., half_dim:]
    return jnp.concatenate([first_half * cosine - second_half * sine_val, second_half * cosine + first_half * sine_val], axis=-1).astype(jnp.bfloat16)


def softmax_mix(scores, key_mask, form, values):
    scores = jnp.where(key_mask, scores, -1e30)
    row_max = jnp.max(scores, axis=-1, keepdims=True)
    weights = jnp.exp(scores - row_max)
    weight_sum = jnp.sum(weights, axis=-1, keepdims=True)
    mixed_out = jnp.einsum(form, weights.astype(jnp.bfloat16).astype(jnp.float32), values)
    return (mixed_out / weight_sum).astype(jnp.bfloat16)


def reference(x_in, req_ids, positions, block_table, ctx_len, k_pages, v_pages, w_q, w_k, w_v, w_o, w_gate, w_up, w_down, g_attn, g_mlp):
    hidden = rms_norm(x_in, g_attn)
    q_rows = jnp.dot(hidden, w_q, preferred_element_type=jnp.float32).astype(jnp.bfloat16).reshape(TOKENS, HEADS, HEAD)
    k_rows = jnp.dot(hidden, w_k, preferred_element_type=jnp.float32).astype(jnp.bfloat16).reshape(TOKENS, KV_HEADS, HEAD)
    v_rows = jnp.dot(hidden, w_v, preferred_element_type=jnp.float32).astype(jnp.bfloat16).reshape(TOKENS, KV_HEADS, HEAD)
    q_rows = rotary(q_rows, positions)
    k_rows = rotary(k_rows, positions)
    page_ids = block_table[req_ids, positions // PAGE]
    slot_ids = positions % PAGE
    k_cache = k_pages.at[page_ids, slot_ids].set(k_rows)
    v_cache = v_pages.at[page_ids, slot_ids].set(v_rows)
    last_key = jnp.minimum(positions, ctx_len[req_ids] - 1)
    key_pos = jnp.arange(TABLE_WIDTH * PAGE)
    attn_scale = HEAD ** -0.5
    chunk_row = block_table[req_ids[0]]
    chunk_keys = k_cache[chunk_row].reshape(TABLE_WIDTH * PAGE, KV_HEADS, HEAD).astype(jnp.float32)
    chunk_vals = v_cache[chunk_row].reshape(TABLE_WIDTH * PAGE, KV_HEADS, HEAD).astype(jnp.float32)

    def chunk_block(block_args):
        q_blk, last_blk = block_args
        scores = jnp.einsum('bgrd,tgd->bgrt', q_blk.astype(jnp.float32), chunk_keys) * attn_scale
        key_mask = (key_pos[None, :] <= last_blk[:, None])[:, None, None, :]
        return softmax_mix(scores, key_mask, 'bgrt,tgd->bgrd', chunk_vals)

    chunk_out = lax.map(chunk_block, (q_rows[:CHUNK].reshape(CHUNK // QUERY_BLOCK, QUERY_BLOCK, KV_HEADS, GROUP_REP, HEAD), last_key[:CHUNK].reshape(CHUNK // QUERY_BLOCK, QUERY_BLOCK)))

    def decode_block(block_args):
        q_blk, req_blk, last_blk = block_args
        rows_blk = block_table[req_blk]
        keys_blk = k_cache[rows_blk].reshape(DECODE_BLOCK, TABLE_WIDTH * PAGE, KV_HEADS, HEAD).astype(jnp.float32)
        vals_blk = v_cache[rows_blk].reshape(DECODE_BLOCK, TABLE_WIDTH * PAGE, KV_HEADS, HEAD).astype(jnp.float32)
        scores = jnp.einsum('bgrd,btgd->bgrt', q_blk.astype(jnp.float32), keys_blk) * attn_scale
        key_mask = (key_pos[None, :] <= last_blk[:, None])[:, None, None, :]
        return softmax_mix(scores, key_mask, 'bgrt,btgd->bgrd', vals_blk)

    dec_blocks = DECODE // DECODE_BLOCK
    dec_out = lax.map(decode_block, (q_rows[CHUNK:].reshape(dec_blocks, DECODE_BLOCK, KV_HEADS, GROUP_REP, HEAD), req_ids[CHUNK:].reshape(dec_blocks, DECODE_BLOCK), last_key[CHUNK:].reshape(dec_blocks, DECODE_BLOCK)))
    attn_rows = jnp.concatenate([chunk_out.reshape(CHUNK, HEADS * HEAD), dec_out.reshape(DECODE, HEADS * HEAD)], axis=0)
    attn_proj = jnp.dot(attn_rows, w_o, preferred_element_type=jnp.float32)
    mid_rows = (x_in.astype(jnp.float32) + attn_proj).astype(jnp.bfloat16)
    hidden_mlp = rms_norm(mid_rows, g_mlp)
    gate_proj = jnp.dot(hidden_mlp, w_gate, preferred_element_type=jnp.float32)
    up_proj = jnp.dot(hidden_mlp, w_up, preferred_element_type=jnp.float32)
    act_rows = (jax.nn.silu(gate_proj) * up_proj).astype(jnp.bfloat16)
    down_proj = jnp.dot(act_rows, w_down, preferred_element_type=jnp.float32)
    x_out = (mid_rows.astype(jnp.float32) + down_proj).astype(jnp.bfloat16)
    return x_out, k_cache, v_cache
```

```python
import functools

import jax
import jax.numpy as jnp
from jax import lax
from jax.experimental import pallas as pl
from jax.experimental.pallas import tpu as pltpu
from jax.sharding import PartitionSpec as P, NamedSharding

EPS = 1e-5
THETA = 500000.0


def rms_norm(rows, gain):
    rows32 = rows.astype(jnp.float32)
    inv_rms = lax.rsqrt(jnp.mean(rows32 * rows32, axis=-1, keepdims=True) + EPS)
    return (rows32 * inv_rms * gain.astype(jnp.float32)).astype(jnp.bfloat16)


def rotary(vals, positions):
    half_dim = vals.shape[-1] // 2
    inv_freq = THETA ** (-jnp.arange(half_dim, dtype=jnp.float32) * 2.0 / vals.shape[-1])
    angles = positions.astype(jnp.float32)[:, None] * inv_freq[None, :]
    cosine = jnp.cos(angles)[:, None, :]
    sine_val = jnp.sin(angles)[:, None, :]
    vals32 = vals.astype(jnp.float32)
    first_half = vals32[..., :half_dim]
    second_half = vals32[..., half_dim:]
    return jnp.concatenate([first_half * cosine - second_half * sine_val, second_half * cosine + first_half * sine_val], axis=-1).astype(jnp.bfloat16)


ATT_CP = dict(vmem_limit_bytes=60 * 1024 * 1024)
LOG2E = 1.4426950408889634


def attend_kernel(dec_len, heads, dec_pages, tab, req, pos, last, q, k_new, v_new, k_in, v_in, o, k_out, v_out, kc, vc, kg, vg, kch, vch, kf, vf, sems):
    tokens, head_dim = k_new.shape
    page_len = kc.shape[1]
    chunk = tokens - dec_len
    span = kch.shape[0]
    prefix = span - chunk
    pre_pages = prefix // page_len
    scale = head_dim ** -0.5 * LOG2E
    r0 = req[0]

    def pull(j, carry):
        page = tab[j, r0]
        rows = pl.ds(pl.multiple_of(j * page_len, page_len), page_len)
        pltpu.make_async_copy(k_in.at[page], kch.at[rows], sems.at[0]).start()
        pltpu.make_async_copy(v_in.at[page], vch.at[rows], sems.at[1]).start()
        return carry

    lax.fori_loop(0, pre_pages, pull, 0)
    load_k = pltpu.make_async_copy(k_in, kc, sems.at[2])
    load_v = pltpu.make_async_copy(v_in, vc, sems.at[3])
    load_k.start()
    load_v.start()
    kch[prefix:, :] = k_new[:chunk, :]
    vch[prefix:, :] = v_new[:chunk, :]
    kf[...] = k_new[chunk:, :].astype(jnp.float32)
    vf[...] = v_new[chunk:, :].astype(jnp.float32)
    pltpu.make_async_copy(kch.at[pl.ds(0, prefix)], kch.at[pl.ds(0, prefix)], sems.at[0]).wait()
    pltpu.make_async_copy(vch.at[pl.ds(0, prefix)], vch.at[pl.ds(0, prefix)], sems.at[1]).wait()

    def nt(a, b):
        return lax.dot_general(a, b, (((1,), (1,)), ((), ())), preferred_element_type=jnp.float32)

    blk = 128
    for b in range(chunk // blk):
        rows = slice(b * blk, (b + 1) * blk)
        full = prefix + b * blk
        qb = jnp.concatenate([q[rows, h * head_dim:(h + 1) * head_dim] for h in range(heads)], axis=0)
        s1 = nt(qb, kch[:full, :])
        s2 = nt(qb, kch[full:full + blk, :])
        row_id = lax.broadcasted_iota(jnp.int32, s2.shape, 0) % blk
        col_id = lax.broadcasted_iota(jnp.int32, s2.shape, 1)
        s2 = jnp.where(col_id <= row_id, s2, -1e30)
        m = jnp.maximum(jnp.max(s1, axis=1, keepdims=True), jnp.max(s2, axis=1, keepdims=True))
        w1 = jnp.exp2((s1 - m) * scale)
        w2 = jnp.exp2((s2 - m) * scale)
        total = jnp.sum(w1, axis=1, keepdims=True) + jnp.sum(w2, axis=1, keepdims=True)
        mix = jnp.dot(w1.astype(jnp.bfloat16), vch[:full, :], preferred_element_type=jnp.float32)
        mix = mix + jnp.dot(w2.astype(jnp.bfloat16), vch[full:full + blk, :], preferred_element_type=jnp.float32)
        ob = (mix / total).astype(jnp.bfloat16)
        for h in range(heads):
            o[rows, h * head_dim:(h + 1) * head_dim] = ob[h * blk:(h + 1) * blk, :]

    load_k.wait()
    load_v.wait()

    def put_page(j, carry):
        page = tab[pre_pages + j, r0]
        rows = pl.ds(pl.multiple_of(j * page_len, page_len), page_len)
        kc[page] = k_new[rows, :]
        vc[page] = v_new[rows, :]
        return carry

    lax.fori_loop(0, chunk // page_len, put_page, 0)
    slot_id = lax.broadcasted_iota(jnp.int32, (page_len, head_dim), 0)

    def put_row(r, carry):
        p = pos[chunk + r]
        page = tab[p // page_len, req[chunk + r]]
        here = slot_id == p % page_len
        kc[page] = jnp.where(here, kf[pl.ds(r, 1), :], kc[page].astype(jnp.float32)).astype(jnp.bfloat16)
        vc[page] = jnp.where(here, vf[pl.ds(r, 1), :], vc[page].astype(jnp.float32)).astype(jnp.bfloat16)
        return carry

    lax.fori_loop(0, dec_len, put_row, 0)
    store_k = pltpu.make_async_copy(kc, k_out, sems.at[2])
    store_v = pltpu.make_async_copy(vc, v_out, sems.at[3])
    store_k.start()
    store_v.start()

    def take(r, carry):
        rid = req[chunk + r]
        for j in range(dec_pages):
            page = tab[j, rid]
            rows = pl.ds(pl.multiple_of((r * dec_pages + j) * page_len, page_len), page_len)
            kg[rows, :] = kc[page]
            vg[rows, :] = vc[page]
        return carry

    lax.fori_loop(0, dec_len, take, 0)
    grp = 16
    dspan = dec_pages * page_len
    for g in range(dec_len // grp):
        rows = slice(chunk + g * grp, chunk + (g + 1) * grp)
        keys = slice(g * grp * dspan, (g + 1) * grp * dspan)
        qb = jnp.concatenate([q[rows, h * head_dim:(h + 1) * head_dim] for h in range(heads)], axis=0)
        s = nt(qb, kg[keys, :])
        lg = last[g * grp:(g + 1) * grp, :]
        low = (lax.broadcasted_iota(jnp.int32, (grp * heads, 1), 0) % grp) * dspan
        high = low + jnp.concatenate([lg] * heads, axis=0)
        col = lax.broadcasted_iota(jnp.int32, s.shape, 1)
        s = jnp.where((col >= low) & (col <= high), s, -1e30)
        m = jnp.max(s, axis=1, keepdims=True)
        w = jnp.exp2((s - m) * scale)
        total = jnp.sum(w, axis=1, keepdims=True)
        mix = jnp.dot(w.astype(jnp.bfloat16), vg[keys, :], preferred_element_type=jnp.float32)
        ob = (mix / total).astype(jnp.bfloat16)
        for h in range(heads):
            o[rows, h * head_dim:(h + 1) * head_dim] = ob[h * grp:(h + 1) * grp, :]
    store_k.wait()
    store_v.wait()


DEC_SPAN = 256


def attend(q, k_new, v_new, positions, req_ids, block_table, ctx_len, k_pages, v_pages):
    tokens, head_dim = k_new.shape
    pages, page_len = k_pages.shape[:2]
    dec_len = block_table.shape[0] - 1
    chunk = tokens - dec_len
    heads = q.shape[1] // head_dim
    span = block_table.shape[1] * page_len
    dec_pages = DEC_SPAN // page_len
    last = jnp.minimum(positions[chunk:], ctx_len[req_ids[chunk:]] - 1)[:, None]
    smem = pl.BlockSpec(memory_space=pltpu.SMEM)
    vmem = pl.BlockSpec(memory_space=pltpu.VMEM)
    hbm = pl.BlockSpec(memory_space=pl.ANY)
    cache = jax.ShapeDtypeStruct((pages, page_len, head_dim), jnp.bfloat16)
    o, k_out, v_out = pl.pallas_call(
        functools.partial(attend_kernel, dec_len, heads, dec_pages),
        out_shape=(jax.ShapeDtypeStruct(q.shape, jnp.bfloat16), cache, cache),
        in_specs=[smem, smem, smem, vmem, vmem, vmem, vmem, hbm, hbm],
        out_specs=(vmem, hbm, hbm),
        scratch_shapes=[
            pltpu.VMEM((pages, page_len, head_dim), jnp.bfloat16),
            pltpu.VMEM((pages, page_len, head_dim), jnp.bfloat16),
            pltpu.VMEM((dec_len * DEC_SPAN, head_dim), jnp.bfloat16),
            pltpu.VMEM((dec_len * DEC_SPAN, head_dim), jnp.bfloat16),
            pltpu.VMEM((span, head_dim), jnp.bfloat16),
            pltpu.VMEM((span, head_dim), jnp.bfloat16),
            pltpu.VMEM((dec_len, head_dim), jnp.float32),
            pltpu.VMEM((dec_len, head_dim), jnp.float32),
            pltpu.SemaphoreType.DMA((4,)),
        ],
        compiler_params=pltpu.CompilerParams(**ATT_CP),
        name="attend",
    )(block_table.T, req_ids, positions, last, q, k_new, v_new, k_pages.reshape(cache.shape), v_pages.reshape(cache.shape))
    return o, k_out.reshape(k_pages.shape), v_out.reshape(v_pages.shape)


def project(hidden, positions, head_dim, w_q, w_k, w_v):
    tokens = hidden.shape[0]
    q_rows = jnp.dot(hidden, w_q, preferred_element_type=jnp.float32).astype(jnp.bfloat16).reshape(tokens, -1, head_dim)
    k_rows = jnp.dot(hidden, w_k, preferred_element_type=jnp.float32).astype(jnp.bfloat16).reshape(tokens, -1, head_dim)
    v_rows = jnp.dot(hidden, w_v, preferred_element_type=jnp.float32).astype(jnp.bfloat16)
    return rotary(q_rows, positions).reshape(tokens, -1), rotary(k_rows, positions).reshape(tokens, -1), v_rows


def solution(mesh):
    row_spec = P(('dp', 'tp'), None)
    group_vec = P('dp')
    table_spec = P('dp', None)
    cache_spec = P('dp', None, 'tp', None)
    col_split = P(None, 'tp')
    row_split = P('tp', None)
    gain_spec = P(None)

    def device_layer(x_in, req_ids, positions, block_table, ctx_len, k_pages, v_pages, w_q, w_k, w_v, w_o, w_gate, w_up, w_down, g_attn, g_mlp):
        hidden = lax.all_gather(rms_norm(x_in, g_attn), 'tp', axis=0, tiled=True)
        q_rows, k_rows, v_rows = project(hidden, positions, k_pages.shape[3], w_q, w_k, w_v)
        attn_rows, k_cache, v_cache = attend(q_rows, k_rows, v_rows, positions, req_ids, block_table, ctx_len, k_pages, v_pages)
        attn_part = jnp.dot(attn_rows, w_o, preferred_element_type=jnp.float32).astype(jnp.bfloat16)
        attn_sum = lax.psum_scatter(attn_part, 'tp', scatter_dimension=0, tiled=True)
        mid_rows = (x_in.astype(jnp.float32) + attn_sum.astype(jnp.float32)).astype(jnp.bfloat16)
        hidden_mlp = lax.all_gather(rms_norm(mid_rows, g_mlp), 'tp', axis=0, tiled=True)
        gate_proj = jnp.dot(hidden_mlp, w_gate, preferred_element_type=jnp.float32)
        up_proj = jnp.dot(hidden_mlp, w_up, preferred_element_type=jnp.float32)
        act_rows = (jax.nn.silu(gate_proj) * up_proj).astype(jnp.bfloat16)
        down_part = jnp.dot(act_rows, w_down, preferred_element_type=jnp.float32).astype(jnp.bfloat16)
        down_sum = lax.psum_scatter(down_part, 'tp', scatter_dimension=0, tiled=True)
        x_out = (mid_rows.astype(jnp.float32) + down_sum.astype(jnp.float32)).astype(jnp.bfloat16)
        return x_out, k_cache, v_cache

    return jax.shard_map(device_layer, mesh=mesh, in_specs=(row_spec, group_vec, group_vec, table_spec, group_vec, cache_spec, cache_spec, col_split, col_split, col_split, row_split, col_split, col_split, row_split, gain_spec, gain_spec), out_specs=(row_spec, cache_spec, cache_spec), check_vma=False)
```
